128 devices in a mesh: rows: 16 (over z, y), cols: 8 (over x, core).
Axes of the slice: x: 4, y: 4, z: 4, core: 2. Of those that a mesh axis runs over, the one named last changes fastest.
Arguments:
- grad_stack: float32 [512, 64, 2048], P(None, 'rows', 'cols'), may hold values from -6 to 6
- moment_stack: float32 [512, 64, 2048], P(None, 'rows', 'cols'), may hold values from -6 to 6
- weight_stack: float32 [512, 64, 2048], P(None, 'rows', 'cols'), may hold values from -0.1875 to 0.1875
Outputs:
- new_weights: float32 [512, 64, 2048], P(None, 'rows', 'cols')
- new_momentum: float32 [512, 64, 2048], P(None, 'rows', 'cols')
The draws below stay inside these ranges and needn't reach their ends.
All inputs are finite; a program needn't handle non-finite values.
Results may differ from the reference program's by a relative error of at most 0.0003.
Values sent between devices are 32-bit elements.
No kernel may reach another device: no remote copies, remote signals or barrier semaphores. Data moves between devices by JAX's collectives and lax.ppermute only.
A program may use at most 128 MiB of HBM per device.

```python
import jax
import jax.numpy as jnp
from jax import lax

SIDE = 64
WIDE = 2048
MATS = 512
ITERS = 5


def block_levels(rng, extent, shards, least, high):
    loudness, own = 1.0, jax.random.fold_in(rng, 6)
    for axis_at, shards_of in shards:
        steps = jnp.exp(jax.random.uniform(jax.random.fold_in(own, axis_at), (shards_of,), jnp.float32, least / len(shards), high / len(shards)))
        loudness = loudness * jnp.repeat(steps, extent[axis_at] // shards_of).reshape([-1 if axis == axis_at else 1 for axis in range(len(extent))])
    return loudness


def centred(own_key, dims, spread, most, cuts=(), dtype=jnp.bfloat16):
    loudness = block_levels(own_key, dims, cuts, -0.22, 0.18) if cuts else 1.0
    array = jax.random.normal(own_key, dims, jnp.float32) * spread * loudness
    return jnp.minimum(jnp.maximum(array, -most), most).astype(dtype)


def setup_inputs(seed: int = 0) -> dict:
    key_list = jax.random.split(jax.random.key(seed), 4)
    return {
        "grad_stack": centred(key_list[0], (MATS, SIDE, WIDE), 1.0, 6.0, ((1, 16), (2, 8)), jnp.float32),
        "moment_stack": centred(key_list[1], (MATS, SIDE, WIDE), 1.0, 6.0, ((1, 16), (2, 8)), jnp.float32),
        "weight_stack": centred(key_list[2], (MATS, SIDE, WIDE), 0.03, 0.1875, ((1, 16), (2, 8)), jnp.float32),
    }


hold_rate = 0.95
learn_rate = 1.0

def reference(grad_stack, moment_stack, weight_stack):
    new_momentum = hold_rate * moment_stack + grad_stack

    def orthogonal_one(stack):
        iterate = stack[None]
        iterate = iterate * lax.rsqrt(lax.optimization_barrier(jnp.sum(iterate * iterate, axis=(1, 2), keepdims=True)) + 1e-06)
        for step in range(ITERS):
            gram = jnp.einsum('mik,mjk->mij', iterate, iterate, precision=lax.Precision.HIGHEST)
            mixed = -4.775 * gram + 2.0315 * jnp.einsum('mij,mjk->mik', gram, gram, precision=lax.Precision.HIGHEST)
            iterate = 3.4445 * iterate + jnp.einsum('mij,mjk->mik', mixed, iterate, precision=lax.Precision.HIGHEST)
        return iterate[0]
    iterate = lax.map(orthogonal_one, new_momentum)
    new_weights = weight_stack - learn_rate * iterate
    return (new_weights, new_momentum)
```

```python
import jax
import jax.numpy as jnp
from jax import lax
from jax.sharding import PartitionSpec as P

ITERS = 5


hold_rate = 0.95
learn_rate = 1.0


def dot(eq, a, b):
    return jnp.einsum(eq, a, b, precision=lax.Precision.HIGHEST)


def on_device(grad_stack, moment_stack, weight_stack):
    new_momentum = hold_rate * moment_stack + grad_stack
    rows_in = lax.all_to_all(new_momentum, "rows", split_axis=0, concat_axis=1, tiled=True)
    part = dot("mik,mjk->mij", rows_in, rows_in)
    n = part.shape[0]
    packed = jnp.concatenate([part[: n // 2], part[n // 2 :]], axis=2)
    parts = lax.all_to_all(packed, "cols", split_axis=0, concat_axis=0, tiled=True)
    k = lax.axis_size("cols")
    total = jnp.sum(parts.reshape(k, n // 2 // k, 64, 128), axis=0)
    gram = jnp.concatenate([total[:, :, :64], total[:, :, 64:]], axis=0)
    size = jnp.trace(gram, axis1=1, axis2=2)[:, None, None] + 1e-06
    gram = gram / size
    eye = jnp.eye(64, dtype=jnp.float32)
    left = lax.rsqrt(size) * eye
    for step in range(ITERS):
        square = dot("mij,mjk->mik", gram, gram)
        poly = 3.4445 * eye - 4.775 * gram + 2.0315 * square
        left = dot("mij,mjk->mik", poly, left)
        if step + 1 < ITERS:
            gram = dot("mij,mjk->mik", poly, dot("mij,mjk->mik", gram, poly))
            gram = 0.5 * (gram + jnp.swapaxes(gram, 1, 2))
    packed = jnp.concatenate([left[: n // 2 // k], left[n // 2 // k :]], axis=2)
    lefts = lax.all_gather(packed, "cols", axis=0, tiled=True)
    lefts = jnp.concatenate([lefts[:, :, :64], lefts[:, :, 64:]], axis=0)
    iterate = dot("mij,mjk->mik", lefts, rows_in)
    back = lax.all_to_all(iterate, "rows", split_axis=1, concat_axis=0, tiled=True)
    new_weights = weight_stack - learn_rate * back
    return (new_weights, new_momentum)


def solution(mesh):
    placed = (P(None, "rows", "cols"), P(None, "rows", "cols"), P(None, "rows", "cols"))
    return jax.shard_map(
        on_device,
        mesh=mesh,
        in_specs=placed,
        out_specs=(P(None, "rows", "cols"), P(None, "rows", "cols")),
        check_vma=False,
    )
```

```python
import jax
import jax.numpy as jnp
from jax import lax
from jax.experimental import pallas as pl
from jax.experimental.pallas import tpu as pltpu
from jax.sharding import PartitionSpec as P

ITERS = 5


hold_rate = 0.95
learn_rate = 1.0


def dot(a, b):
    return lax.dot_general(
        a, b, (((1,), (0,)), ((), ())),
        precision=lax.Precision.HIGHEST, preferred_element_type=jnp.float32,
    )


def dot_t(a, b):
    return lax.dot_general(
        a, b, (((1,), (1,)), ((), ())),
        precision=lax.Precision.HIGHEST, preferred_element_type=jnp.float32,
    )


def orthogonal(rows, cols, mats):
    def body(in_ref, out_ref, x_ref, left_ref):
        here, wide = in_ref.shape[1], in_ref.shape[2]
        side = here * rows
        for m in range(mats):
            for r in range(0, rows, 2):
                for c in range(cols):
                    top = in_ref[(r * cols + c) * mats + m]
                    low = in_ref[((r + 1) * cols + c) * mats + m]
                    x_ref[m, pl.ds(r * here, 2 * here), pl.ds(c * wide, wide)] = jnp.concatenate([top, low], axis=0)
        at_row = lax.broadcasted_iota(jnp.int32, (side, side), 0)
        at_col = lax.broadcasted_iota(jnp.int32, (side, side), 1)
        eye = jnp.where(at_row == at_col, 1.0, 0.0).astype(jnp.float32)
        grams, lefts = [], []
        for m in range(mats):
            x = x_ref[m]
            gram = dot_t(x, x)
            size = jnp.sum(gram * eye, axis=(0, 1), keepdims=True) + 1e-06
            grams.append(gram / size)
            lefts.append(lax.rsqrt(size) * eye)
        for step in range(ITERS):
            squares = [dot(g, g) for g in grams]
            polys = [3.4445 * eye - 4.775 * g + 2.0315 * s for g, s in zip(grams, squares)]
            lefts = [dot(p, q) for p, q in zip(polys, lefts)]
            if step + 1 < ITERS:
                halves = [dot(g, p) for g, p in zip(grams, polys)]
                grams = [dot(p, h) for p, h in zip(polys, halves)]
                grams = [0.5 * (g + g.T) for g in grams]
        for m in range(mats):
            y = dot(lefts[m], x_ref[m])
            for r in range(rows):
                for c in range(cols):
                    out_ref[(r * cols + c) * mats + m] = y[r * here : (r + 1) * here, c * wide : (c + 1) * wide]

    def call(pieces):
        n, here, wide = pieces.shape
        return pl.pallas_call(
            body,
            out_shape=jax.ShapeDtypeStruct(pieces.shape, pieces.dtype),
            in_specs=[pl.BlockSpec(memory_space=pltpu.VMEM)],
            out_specs=pl.BlockSpec(memory_space=pltpu.VMEM),
            scratch_shapes=[
                pltpu.VMEM((mats, here * rows, wide * cols), jnp.float32),
                pltpu.VMEM((mats, here * rows, here * rows), jnp.float32),
            ],
            compiler_params=pltpu.CompilerParams(vmem_limit_bytes=32 * 1024 * 1024),
            name="orthogonal",
        )(pieces)

    return call


def on_device(grad_stack, moment_stack, weight_stack):
    axes = ("rows", "cols")
    rows, cols = lax.axis_size("rows"), lax.axis_size("cols")
    new_momentum = hold_rate * moment_stack + grad_stack
    pieces = lax.all_to_all(new_momentum, axes, split_axis=0, concat_axis=0, tiled=True)
    pieces = orthogonal(rows, cols, pieces.shape[0] // (rows * cols))(pieces)
    back = lax.all_to_all(pieces, axes, split_axis=0, concat_axis=0, tiled=True)
    new_weights = weight_stack - learn_rate * back
    return (new_weights, new_momentum)


def solution(mesh):
    placed = (P(None, "rows", "cols"), P(None, "rows", "cols"), P(None, "rows", "cols"))
    return jax.shard_map(
        on_device,
        mesh=mesh,
        in_specs=placed,
        out_specs=(P(None, "rows", "cols"), P(None, "rows", "cols")),
        check_vma=False,
    )
```

```python
import jax
import jax.numpy as jnp
from jax import lax
from jax.experimental import pallas as pl
from jax.experimental.pallas import tpu as pltpu
from jax.sharding import PartitionSpec as P

ITERS = 5
RESTART = 3


hold_rate = 0.95
learn_rate = 1.0

F32, BF16 = jnp.float32, jnp.bfloat16


def split3(value):
    high = value.astype(BF16)
    rest = value - high.astype(F32)
    mid = rest.astype(BF16)
    return high, mid, (rest - mid.astype(F32)).astype(BF16)


def dot(a, b):
    return lax.dot_general(a, b, (((1,), (0,)), ((), ())), preferred_element_type=F32)


def dot_t(a, b):
    return lax.dot_general(a, b, (((1,), (1,)), ((), ())), preferred_element_type=F32)


def orthogonal(rows, cols, mats):
    def body(in_ref, out_ref, x_ref):
        here, wide = in_ref.shape[1], in_ref.shape[2]
        side = here * rows
        lane = lax.broadcasted_iota(jnp.int32, (side, 2 * side), 1)
        row = lax.broadcasted_iota(jnp.int32, (side, 2 * side), 0)
        eye = jnp.where((lane == row) | (lane == row + side), 1.0, 0.0).astype(F32)
        eye_one = eye[:, :side]
        first = jnp.where(lane < side, 1.0, 0.0).astype(BF16)
        second = jnp.where(lane < side, 0.0, 1.0).astype(BF16)

        def keep(m, top, at, value):
            for k, term in enumerate(split3(value)):
                x_ref[m, pl.ds(k * side + top, value.shape[0]), pl.ds(at, value.shape[1])] = term

        def gram_of(m):
            c = dot_t(x_ref[m, : 2 * side], x_ref[m])
            half = c[:side, side : 2 * side] + (c[:side, 2 * side :] + 0.5 * c[side:, side : 2 * side])
            return c[:side, :side] + (half + half.T)

        def streamed(value):
            v1, v2, v3 = split3(value)
            return jnp.concatenate([v1, v1, v1, v2, v2, v3], axis=1)

        def held(value):
            v1, v2, v3 = [jnp.concatenate([v * first, v * second], axis=0) for v in split3(value)]
            return jnp.concatenate([v1, v2, v3, v1, v2, v1], axis=0)

        def steps(grams, lefts, count):
            pairs = range(len(grams))
            for step in range(count):
                gram_held = [held(g) for g in grams]
                squares = [dot(streamed(grams[p]), gram_held[p]) for p in pairs]
                polys = [3.4445 * eye - 4.775 * grams[p] + 2.0315 * squares[p] for p in pairs]
                flow = [streamed(poly) for poly in polys]
                last = step + 1 == count
                if step == 0:
                    mixed = None if last else [dot(flow[p], gram_held[p]) for p in pairs]
                    lefts = [polys[p] if lefts is None else polys[p] * lefts[p] for p in pairs]
                elif last:
                    lefts = [dot(flow[p], held(lefts[p])) for p in pairs]
                else:
                    both = [dot(flow[p], jnp.concatenate([held(lefts[p]), gram_held[p]], axis=1)) for p in pairs]
                    lefts = [b[:, : 2 * side] for b in both]
                    mixed = [b[:, 2 * side :] for b in both]
                if not last:
                    grams = [dot(streamed(mixed[p]), held(polys[p])) for p in pairs]
            return lefts

        def weights_of(lefts, m):
            left = lefts[m // 2][:, (m % 2) * side : (m % 2 + 1) * side]
            q1, q2, q3 = split3(left)
            none = jnp.zeros((side, 2 * side), BF16)
            return jnp.concatenate(
                [jnp.concatenate([q1, q1, q1, q2], axis=1), jnp.concatenate([q3, q2, none], axis=1)], axis=0
            )

        def applied(weights, m, at):
            terms = x_ref[m, :, pl.ds(at, wide)]
            got = dot(weights, jnp.concatenate([terms, terms[:side]], axis=0))
            return got[:side] + got[side:]

        def pair_up(values):
            return [jnp.concatenate(values[m : m + 2], axis=1) for m in range(0, mats, 2)]

        for m in range(mats):
            for r in range(0, rows, 4):
                for c in range(cols):
                    piece = [in_ref[((r + k) * cols + c) * mats + m] for k in range(4)]
                    keep(m, r * here, c * wide, jnp.concatenate(piece, axis=0))
        grams = [gram_of(m) for m in range(mats)]
        sizes = [jnp.sum(g * eye_one, axis=(0, 1), keepdims=True) + 1e-06 for g in grams]
        scales = [jnp.broadcast_to(lax.rsqrt(s), (side, side)) for s in sizes]
        grams = [g / s for g, s in zip(grams, sizes)]
        lefts = steps(pair_up(grams), pair_up(scales), RESTART)
        for m in range(mats):
            weights = weights_of(lefts, m)
            for c in range(cols):
                keep(m, 0, c * wide, applied(weights, m, c * wide))
        lefts = steps(pair_up([gram_of(m) for m in range(mats)]), None, ITERS - RESTART)
        for m in range(mats):
            weights = weights_of(lefts, m)
            for c in range(cols):
                y = applied(weights, m, c * wide)
                for r in range(rows):
                    out_ref[(r * cols + c) * mats + m] = y[r * here : (r + 1) * here]

    def call(pieces):
        n, here, wide = pieces.shape
        return pl.pallas_call(
            body,
            out_shape=jax.ShapeDtypeStruct(pieces.shape, pieces.dtype),
            in_specs=[pl.BlockSpec(memory_space=pltpu.VMEM)],
            out_specs=pl.BlockSpec(memory_space=pltpu.VMEM),
            scratch_shapes=[pltpu.VMEM((mats, 3 * here * rows, wide * cols), BF16)],
            compiler_params=pltpu.CompilerParams(vmem_limit_bytes=32 * 1024 * 1024),
            name="orthogonal",
        )(pieces)

    return call


def on_device(grad_stack, moment_stack, weight_stack):
    axes = ("rows", "cols")
    rows, cols = lax.axis_size("rows"), lax.axis_size("cols")
    new_momentum = hold_rate * moment_stack + grad_stack
    pieces = lax.all_to_all(new_momentum, axes, split_axis=0, concat_axis=0, tiled=True)
    pieces = orthogonal(rows, cols, pieces.shape[0] // (rows * cols))(pieces)
    back = lax.all_to_all(pieces, axes, split_axis=0, concat_axis=0, tiled=True)
    new_weights = weight_stack - learn_rate * back
    return (new_weights, new_momentum)


def solution(mesh):
    placed = (P(None, "rows", "cols"), P(None, "rows", "cols"), P(None, "rows", "cols"))
    return jax.shard_map(
        on_device,
        mesh=mesh,
        in_specs=placed,
        out_specs=(P(None, "rows", "cols"), P(None, "rows", "cols")),
        check_vma=False,
    )
```

```python
import jax
import jax.numpy as jnp
from jax import lax
from jax.experimental import pallas as pl
from jax.experimental.pallas import tpu as pltpu
from jax.sharding import PartitionSpec as P

ITERS = 5
RESTART = 3


hold_rate = 0.95
learn_rate = 1.0

F32, BF16 = jnp.float32, jnp.bfloat16


def split3(value):
    high = value.astype(BF16)
    rest = value - high.astype(F32)
    mid = rest.astype(BF16)
    return high, mid, (rest - mid.astype(F32)).astype(BF16)


def dot(a, b):
    return lax.dot_general(a, b, (((1,), (0,)), ((), ())), preferred_element_type=F32)


def dot_t(a, b):
    return lax.dot_general(a, b, (((1,), (1,)), ((), ())), preferred_element_type=F32)


def orthogonal(rows, cols, mats):
    def body(in_ref, kept_ref, out_ref, kept_out_ref, x_ref, written):
        here, wide = in_ref.shape[1], in_ref.shape[2]
        side = here * rows
        lane = lax.broadcasted_iota(jnp.int32, (side, 2 * side), 1)
        row = lax.broadcasted_iota(jnp.int32, (side, 2 * side), 0)
        eye = jnp.where((lane == row) | (lane == row + side), 1.0, 0.0).astype(F32)
        eye_one = eye[:, :side]
        first = jnp.where(lane < side, 1.0, 0.0).astype(BF16)
        second = jnp.where(lane < side, 0.0, 1.0).astype(BF16)

        def keep(m, top, at, value):
            for k, term in enumerate(split3(value)):
                x_ref[m, pl.ds(k * side + top, value.shape[0]), pl.ds(at, value.shape[1])] = term

        def gram_of(m):
            c = dot_t(x_ref[m, : 2 * side], x_ref[m])
            half = c[:side, side : 2 * side] + (c[:side, 2 * side :] + 0.5 * c[side:, side : 2 * side])
            return c[:side, :side] + (half + half.T)

        def streamed(value):
            v1, v2, v3 = split3(value)
            return jnp.concatenate([v1, v1, v1, v2, v2, v3], axis=1)

        def held(value):
            v1, v2, v3 = [jnp.concatenate([v * first, v * second], axis=0) for v in split3(value)]
            return jnp.concatenate([v1, v2, v3, v1, v2, v1], axis=0)

        def steps(grams, lefts, count):
            pairs = range(len(grams))
            for step in range(count):
                gram_held = [held(g) for g in grams]
                squares = [dot(streamed(grams[p]), gram_held[p]) for p in pairs]
                polys = [3.4445 * eye - 4.775 * grams[p] + 2.0315 * squares[p] for p in pairs]
                flow = [streamed(poly) for poly in polys]
                last = step + 1 == count
                if step == 0:
                    mixed = None if last else [dot(flow[p], gram_held[p]) for p in pairs]
                    lefts = [polys[p] if lefts is None else polys[p] * lefts[p] for p in pairs]
                elif last:
                    lefts = [dot(flow[p], held(lefts[p])) for p in pairs]
                else:
                    both = [dot(flow[p], jnp.concatenate([held(lefts[p]), gram_held[p]], axis=1)) for p in pairs]
                    lefts = [b[:, : 2 * side] for b in both]
                    mixed = [b[:, 2 * side :] for b in both]
                if not last:
                    grams = [dot(streamed(mixed[p]), held(polys[p])) for p in pairs]
            return lefts

        def weights_of(lefts, m):
            left = lefts[m // 2][:, (m % 2) * side : (m % 2 + 1) * side]
            q1, q2, q3 = split3(left)
            none = jnp.zeros((side, 2 * side), BF16)
            return jnp.concatenate(
                [jnp.concatenate([q1, q1, q1, q2], axis=1), jnp.concatenate([q3, q2, none], axis=1)], axis=0
            )

        def applied(weights, m, at):
            terms = x_ref[m, :, pl.ds(at, wide)]
            got = dot(weights, jnp.concatenate([terms, terms[:side]], axis=0))
            return got[:side] + got[side:]

        def pair_up(values):
            return [jnp.concatenate(values[m : m + 2], axis=1) for m in range(0, mats, 2)]

        kept_copy = pltpu.make_async_copy(kept_ref, kept_out_ref, written)
        kept_copy.start()
        for m in range(mats):
            for r in range(0, rows, 4):
                for c in range(cols):
                    piece = [in_ref[((r + k) * cols + c) * mats + m] for k in range(4)]
                    keep(m, r * here, c * wide, jnp.concatenate(piece, axis=0))
        grams = [gram_of(m) for m in range(mats)]
        sizes = [jnp.sum(g * eye_one, axis=(0, 1), keepdims=True) + 1e-06 for g in grams]
        scales = [jnp.broadcast_to(lax.rsqrt(s), (side, side)) for s in sizes]
        grams = [g / s for g, s in zip(grams, sizes)]
        lefts = steps(pair_up(grams), pair_up(scales), RESTART)
        for m in range(mats):
            weights = weights_of(lefts, m)
            for c in range(cols):
                keep(m, 0, c * wide, applied(weights, m, c * wide))
        lefts = steps(pair_up([gram_of(m) for m in range(mats)]), None, ITERS - RESTART)
        for m in range(mats):
            weights = weights_of(lefts, m)
            for c in range(cols):
                y = applied(weights, m, c * wide)
                for r in range(rows):
                    out_ref[(r * cols + c) * mats + m] = y[r * here : (r + 1) * here]
        kept_copy.wait()

    def call(pieces, kept):
        n, here, wide = pieces.shape
        return pl.pallas_call(
            body,
            out_shape=(
                jax.ShapeDtypeStruct(pieces.shape, pieces.dtype),
                jax.ShapeDtypeStruct(kept.shape, kept.dtype),
            ),
            in_specs=[pl.BlockSpec(memory_space=pltpu.VMEM)] * 2,
            out_specs=(pl.BlockSpec(memory_space=pltpu.VMEM), pl.BlockSpec(memory_space=pltpu.HBM)),
            scratch_shapes=[
                pltpu.VMEM((mats, 3 * here * rows, wide * cols), BF16),
                pltpu.SemaphoreType.DMA,
            ],
            compiler_params=pltpu.CompilerParams(vmem_limit_bytes=32 * 1024 * 1024),
            name="orthogonal",
        )(pieces, kept)

    return call


PARTS = 8


def fresh_momentum(grad_stack, moment_stack):
    many = grad_stack.shape[0] // PARTS

    def body(grad_ref, moment_ref, out_ref, grads, moments, arrived):
        def copies(i):
            part = pl.ds(i * many, many)
            return (
                pltpu.make_async_copy(grad_ref.at[part], grads.at[part], arrived.at[2 * i]),
                pltpu.make_async_copy(moment_ref.at[part], moments.at[part], arrived.at[2 * i + 1]),
            )

        for i in range(PARTS):
            for copy in copies(i):
                copy.start()
        for i in range(PARTS):
            for copy in copies(i):
                copy.wait()
            part = pl.ds(i * many, many)
            out_ref[part] = hold_rate * moments[part] + grads[part]

    return pl.pallas_call(
        body,
        out_shape=pltpu.VMEM(grad_stack.shape, F32),
        in_specs=[pl.BlockSpec(memory_space=pltpu.HBM)] * 2,
        out_specs=pl.BlockSpec(memory_space=pltpu.VMEM),
        scratch_shapes=[
            pltpu.VMEM(grad_stack.shape, F32),
            pltpu.VMEM(grad_stack.shape, F32),
            pltpu.SemaphoreType.DMA((2 * PARTS,)),
        ],
        compiler_params=pltpu.CompilerParams(vmem_limit_bytes=61 * 1024 * 1024),
        name="fresh_momentum",
    )(grad_stack, moment_stack)


def stepped(weight_stack, back):
    many = back.shape[0] // PARTS

    def body(weight_ref, back_ref, out_ref, made, sent):
        def copy(i):
            part = pl.ds(i * many, many)
            return pltpu.make_async_copy(made.at[part], out_ref.at[part], sent.at[i])

        for i in range(PARTS):
            part = pl.ds(i * many, many)
            made[part] = weight_ref[part] - learn_rate * back_ref[part]
            copy(i).start()
        for i in range(PARTS):
            copy(i).wait()

    return pl.pallas_call(
        body,
        out_shape=jax.ShapeDtypeStruct(back.shape, F32),
        in_specs=[pl.BlockSpec(memory_space=pltpu.VMEM)] * 2,
        out_specs=pl.BlockSpec(memory_space=pltpu.HBM),
        scratch_shapes=[pltpu.VMEM(back.shape, F32), pltpu.SemaphoreType.DMA((PARTS,))],
        compiler_params=pltpu.CompilerParams(vmem_limit_bytes=16 * 1024 * 1024),
        name="stepped",
    )(weight_stack, back)


def on_device(grad_stack, moment_stack, weight_stack):
    axes = ("rows", "cols")
    rows, cols = lax.axis_size("rows"), lax.axis_size("cols")
    new_momentum = fresh_momentum(grad_stack, moment_stack)
    pieces = lax.all_to_all(new_momentum, axes, split_axis=0, concat_axis=0, tiled=True)
    pieces, written = orthogonal(rows, cols, pieces.shape[0] // (rows * cols))(pieces, new_momentum)
    back = lax.all_to_all(pieces, axes, split_axis=0, concat_axis=0, tiled=True)
    return (stepped(weight_stack, back), written)


def solution(mesh):
    placed = (P(None, "rows", "cols"), P(None, "rows", "cols"), P(None, "rows", "cols"))
    return jax.shard_map(
        on_device,
        mesh=mesh,
        in_specs=placed,
        out_specs=(P(None, "rows", "cols"), P(None, "rows", "cols")),
        check_vma=False,
    )
```

```python
import jax
import jax.numpy as jnp
from jax import lax
from jax.experimental import pallas as pl
from jax.experimental.pallas import tpu as pltpu
from jax.sharding import PartitionSpec as P

ITERS = 5
RESTART = 3


hold_rate = 0.95
learn_rate = 1.0

F32, BF16 = jnp.float32, jnp.bfloat16


def split3(value):
    high = value.astype(BF16)
    rest = value - high.astype(F32)
    mid = rest.astype(BF16)
    return high, mid, (rest - mid.astype(F32)).astype(BF16)


def dot(a, b):
    return lax.dot_general(a, b, (((1,), (0,)), ((), ())), preferred_element_type=F32)


def dot_t(a, b):
    return lax.dot_general(a, b, (((1,), (1,)), ((), ())), preferred_element_type=F32)


def orthogonal(rows, cols, mats):
    def body(in_ref, kept_ref, out_ref, kept_out_ref, x_ref, written):
        here, wide = in_ref.shape[1], in_ref.shape[2]
        side = here * rows
        lane = lax.broadcasted_iota(jnp.int32, (side, 2 * side), 1)
        row = lax.broadcasted_iota(jnp.int32, (side, 2 * side), 0)
        eye = jnp.where((lane == row) | (lane == row + side), 1.0, 0.0).astype(F32)
        first = jnp.where(lane < side, 1.0, 0.0).astype(BF16)
        second = jnp.where(lane < side, 0.0, 1.0).astype(BF16)

        def keep(m, top, at, value):
            for k, term in enumerate(split3(value)):
                x_ref[m, pl.ds(k * side + top, value.shape[0]), pl.ds(at, value.shape[1])] = term

        def pair_gram(m):
            def by_term(k, order):
                terms = jnp.concatenate([x_ref[k, pl.ds(t * side, side)] for t in order], axis=0)
                c = dot_t(x_ref[k], terms)
                c = c[:side] + (c[side : 2 * side] + c[2 * side :])
                tail = jnp.concatenate([c[:, 2 * side :], jnp.zeros((side, side), F32)], axis=1)
                return c[:, : 2 * side] + tail

            one, two = by_term(m, (0, 1, 2)), by_term(m + 1, (1, 0, 2))
            return jnp.where(lane < side, one, two) + pltpu.roll(jnp.where(lane < side, two, one), side, 1)

        def streamed(value):
            v1, v2, v3 = split3(value)
            return jnp.concatenate([v1, v1, v1, v2, v2, v3], axis=1)

        def held(value):
            v1, v2, v3 = [jnp.concatenate([v * first, v * second], axis=0) for v in split3(value)]
            return jnp.concatenate([v1, v2, v3, v1, v2, v1], axis=0)

        def steps(grams, count, normed):
            pairs = range(len(grams))
            for step in range(count):
                gram_held = [held(g) for g in grams]
                squares = [dot(streamed(grams[p]), gram_held[p]) for p in pairs]
                if step == 0 and normed:
                    sizes = [norms(g) for g in grams]
                    shrink = [1.0 / s for s in sizes]
                    polys = [
                        3.4445 * eye - (4.775 * shrink[p]) * grams[p] + (2.0315 * shrink[p]) * (shrink[p] * squares[p])
                        for p in pairs
                    ]
                else:
                    polys = [3.4445 * eye - 4.775 * grams[p] + 2.0315 * squares[p] for p in pairs]
                flow = [streamed(poly) for poly in polys]
                last = step + 1 == count
                if step == 0:
                    mixed = None if last else [dot(flow[p], gram_held[p]) for p in pairs]
                    lefts = polys
                    if normed:
                        lefts = [poly * lax.rsqrt(s) for poly, s in zip(polys, sizes)]
                        mixed = None if last else [shrink[p] * mixed[p] for p in pairs]
                elif last:
                    lefts = [dot(flow[p], held(lefts[p])) for p in pairs]
                else:
                    both = [dot(flow[p], jnp.concatenate([held(lefts[p]), gram_held[p]], axis=1)) for p in pairs]
                    lefts = [b[:, : 2 * side] for b in both]
                    mixed = [b[:, 2 * side :] for b in both]
                if not last:
                    grams = [dot(streamed(mixed[p]), held(polys[p])) for p in pairs]
            return lefts

        def norms(gram):
            diagonal = jnp.sum(gram * eye, axis=0, keepdims=True)
            one = jnp.sum(jnp.where(lane[:1] < side, diagonal, 0.0), axis=1, keepdims=True)
            two = jnp.sum(jnp.where(lane[:1] < side, 0.0, diagonal), axis=1, keepdims=True)
            return jnp.where(lane[:1] < side, one, two) + 1e-06

        def weights_of(lefts, m):
            left = lefts[m // 2]
            own = lane < side if m % 2 == 0 else lane >= side
            q1, q2, q3 = split3(jnp.where(own, left, pltpu.roll(left, side, 1)))
            after = jnp.concatenate([q2 * second + q1 * first, jnp.zeros_like(q1)], axis=0)
            low = jnp.concatenate([q1, q3 * first + q2 * second], axis=0)
            return jnp.concatenate([low, after], axis=1)

        def applied(weights, m, at):
            terms = x_ref[m, :, pl.ds(at, wide)]
            got = dot(weights, jnp.concatenate([terms, terms[:side]], axis=0))
            return got[:side] + got[side:]

        kept_copy = pltpu.make_async_copy(kept_ref, kept_out_ref, written)
        kept_copy.start()
        for m in range(mats):
            for r in range(0, rows, 4):
                for c in range(cols):
                    piece = [in_ref[((r + k) * cols + c) * mats + m] for k in range(4)]
                    keep(m, r * here, c * wide, jnp.concatenate(piece, axis=0))
        lefts = steps([pair_gram(m) for m in range(0, mats, 2)], RESTART, True)
        for m in range(mats):
            weights = weights_of(lefts, m)
            for c in range(cols):
                keep(m, 0, c * wide, applied(weights, m, c * wide))
        lefts = steps([pair_gram(m) for m in range(0, mats, 2)], ITERS - RESTART, False)
        for m in range(mats):
            weights = weights_of(lefts, m)
            for c in range(cols):
                y = applied(weights, m, c * wide)
                for r in range(rows):
                    out_ref[(r * cols + c) * mats + m] = y[r * here : (r + 1) * here]
        kept_copy.wait()

    def call(pieces, kept):
        n, here, wide = pieces.shape
        return pl.pallas_call(
            body,
            out_shape=(
                jax.ShapeDtypeStruct(pieces.shape, pieces.dtype),
                jax.ShapeDtypeStruct(kept.shape, kept.dtype),
            ),
            in_specs=[pl.BlockSpec(memory_space=pltpu.VMEM)] * 2,
            out_specs=(pl.BlockSpec(memory_space=pltpu.VMEM), pl.BlockSpec(memory_space=pltpu.HBM)),
            scratch_shapes=[
                pltpu.VMEM((mats, 3 * here * rows, wide * cols), BF16),
                pltpu.SemaphoreType.DMA,
            ],
            compiler_params=pltpu.CompilerParams(vmem_limit_bytes=32 * 1024 * 1024),
            name="orthogonal",
        )(pieces, kept)

    return call


PARTS = 8


def fresh_momentum(grad_stack, moment_stack):
    many = grad_stack.shape[0] // PARTS

    def body(grad_ref, moment_ref, out_ref, grads, moments, arrived):
        def copies(i):
            part = pl.ds(i * many, many)
            return (
                pltpu.make_async_copy(grad_ref.at[part], grads.at[part], arrived.at[2 * i]),
                pltpu.make_async_copy(moment_ref.at[part], moments.at[part], arrived.at[2 * i + 1]),
            )

        for i in range(PARTS):
            for copy in copies(i):
                copy.start()
        for i in range(PARTS):
            for copy in copies(i):
                copy.wait()
            part = pl.ds(i * many, many)
            out_ref[part] = hold_rate * moments[part] + grads[part]

    return pl.pallas_call(
        body,
        out_shape=pltpu.VMEM(grad_stack.shape, F32),
        in_specs=[pl.BlockSpec(memory_space=pltpu.HBM)] * 2,
        out_specs=pl.BlockSpec(memory_space=pltpu.VMEM),
        scratch_shapes=[
            pltpu.VMEM(grad_stack.shape, F32),
            pltpu.VMEM(grad_stack.shape, F32),
            pltpu.SemaphoreType.DMA((2 * PARTS,)),
        ],
        compiler_params=pltpu.CompilerParams(vmem_limit_bytes=61 * 1024 * 1024),
        name="fresh_momentum",
    )(grad_stack, moment_stack)


def stepped(weight_stack, back):
    many = back.shape[0] // PARTS

    def body(weight_ref, back_ref, out_ref, made, sent):
        def copy(i):
            part = pl.ds(i * many, many)
            return pltpu.make_async_copy(made.at[part], out_ref.at[part], sent.at[i])

        for i in range(PARTS):
            part = pl.ds(i * many, many)
            made[part] = weight_ref[part] - learn_rate * back_ref[part]
            copy(i).start()
        for i in range(PARTS):
            copy(i).wait()

    return pl.pallas_call(
        body,
        out_shape=jax.ShapeDtypeStruct(back.shape, F32),
        in_specs=[pl.BlockSpec(memory_space=pltpu.VMEM)] * 2,
        out_specs=pl.BlockSpec(memory_space=pltpu.HBM),
        scratch_shapes=[pltpu.VMEM(back.shape, F32), pltpu.SemaphoreType.DMA((PARTS,))],
        compiler_params=pltpu.CompilerParams(vmem_limit_bytes=16 * 1024 * 1024),
        name="stepped",
    )(weight_stack, back)


def on_device(grad_stack, moment_stack, weight_stack):
    axes = ("rows", "cols")
    rows, cols = lax.axis_size("rows"), lax.axis_size("cols")
    new_momentum = fresh_momentum(grad_stack, moment_stack)
    pieces = lax.all_to_all(new_momentum, axes, split_axis=0, concat_axis=0, tiled=True)
    pieces, written = orthogonal(rows, cols, pieces.shape[0] // (rows * cols))(pieces, new_momentum)
    back = lax.all_to_all(pieces, axes, split_axis=0, concat_axis=0, tiled=True)
    return (stepped(weight_stack, back), written)


def solution(mesh):
    placed = (P(None, "rows", "cols"), P(None, "rows", "cols"), P(None, "rows", "cols"))
    return jax.shard_map(
        on_device,
        mesh=mesh,
        in_specs=placed,
        out_specs=(P(None, "rows", "cols"), P(None, "rows", "cols")),
        check_vma=False,
    )
```

```python
import jax
import jax.numpy as jnp
from jax import lax
from jax.experimental import pallas as pl
from jax.experimental.pallas import tpu as pltpu
from jax.sharding import PartitionSpec as P

ITERS = 5
RESTART = 3


hold_rate = 0.95
learn_rate = 1.0

F32, BF16 = jnp.float32, jnp.bfloat16


def split3(value):
    high = value.astype(BF16)
    rest = value - high.astype(F32)
    mid = rest.astype(BF16)
    return high, mid, (rest - mid.astype(F32)).astype(BF16)


def dot(a, b):
    return lax.dot_general(a, b, (((1,), (0,)), ((), ())), preferred_element_type=F32)


def dot_t(a, b):
    return lax.dot_general(a, b, (((1,), (1,)), ((), ())), preferred_element_type=F32)


def orthogonal(rows, cols, mats):
    def body(in_ref, kept_ref, out_ref, kept_out_ref, x_ref, written):
        here, wide = in_ref.shape[1], in_ref.shape[2]
        side = here * rows
        lane = lax.broadcasted_iota(jnp.int32, (side, 2 * side), 1)
        row = lax.broadcasted_iota(jnp.int32, (side, 2 * side), 0)
        eye = jnp.where((lane == row) | (lane == row + side), 1.0, 0.0).astype(F32)
        first = jnp.where(lane < side, 1.0, 0.0).astype(BF16)
        second = jnp.where(lane < side, 0.0, 1.0).astype(BF16)

        def keep(m, top, at, value, terms):
            for k, term in enumerate(split3(value)[:terms]):
                x_ref[m, pl.ds(k * side + top, value.shape[0]), pl.ds(at, value.shape[1])] = term

        def pair_gram(m, terms):
            def by_term(k, order):
                held_terms = jnp.concatenate([x_ref[k, pl.ds(t * side, side)] for t in order], axis=0)
                c = dot_t(x_ref[k, : terms * side], held_terms)
                if terms == 2:
                    return c[:side] + c[side:]
                c = c[:side] + (c[side : 2 * side] + c[2 * side :])
                tail = jnp.concatenate([c[:, 2 * side :], jnp.zeros((side, side), F32)], axis=1)
                return c[:, : 2 * side] + tail

            one, two = by_term(m, (0, 1, 2)[:terms]), by_term(m + 1, (1, 0, 2)[:terms])
            return jnp.where(lane < side, one, two) + pltpu.roll(jnp.where(lane < side, two, one), side, 1)

        def streamed(value):
            v1, v2, v3 = split3(value)
            return jnp.concatenate([v1, v2, v3, v1], axis=1)

        def held(value):
            v1, v2, v3 = [jnp.concatenate([v * first, v * second], axis=0) for v in split3(value)]
            high = jnp.concatenate([v1, v2], axis=1)
            return jnp.concatenate([high, high], axis=0), jnp.concatenate([v1, v3], axis=0)

        def product(flow, weights):
            high = dot(flow[:, : 4 * side], weights[0])
            return high[:, : 2 * side] + (high[:, 2 * side :] + dot(flow[:, 4 * side :], weights[1]))

        def steps(grams, count, normed):
            pairs = range(len(grams))
            for step in range(count):
                gram_held = [held(g) for g in grams]
                squares = [product(streamed(grams[p]), gram_held[p]) for p in pairs]
                if step == 0 and normed:
                    sizes = [norms(g) for g in grams]
                    shrink = [1.0 / s for s in sizes]
                    polys = [
                        3.4445 * eye - (4.775 * shrink[p]) * grams[p] + (2.0315 * shrink[p]) * (shrink[p] * squares[p])
                        for p in pairs
                    ]
                else:
                    polys = [3.4445 * eye - 4.775 * grams[p] + 2.0315 * squares[p] for p in pairs]
                flow = [streamed(poly) for poly in polys]
                last = step + 1 == count
                if step == 0:
                    mixed = None if last else [product(flow[p], gram_held[p]) for p in pairs]
                    lefts = polys
                    if normed:
                        lefts = [poly * lax.rsqrt(s) for poly, s in zip(polys, sizes)]
                        mixed = None if last else [shrink[p] * mixed[p] for p in pairs]
                elif last:
                    lefts = [product(flow[p], held(lefts[p])) for p in pairs]
                else:
                    mixed = [product(flow[p], gram_held[p]) for p in pairs]
                    lefts = [product(flow[p], held(lefts[p])) for p in pairs]
                if not last:
                    grams = [product(streamed(mixed[p]), held(polys[p])) for p in pairs]
            return lefts

        def norms(gram):
            diagonal = jnp.sum(gram * eye, axis=0, keepdims=True)
            one = jnp.sum(jnp.where(lane[:1] < side, diagonal, 0.0), axis=1, keepdims=True)
            two = jnp.sum(jnp.where(lane[:1] < side, 0.0, diagonal), axis=1, keepdims=True)
            return jnp.where(lane[:1] < side, one, two) + 1e-06

        def weights_of(lefts, m, terms):
            left = lefts[m // 2]
            own = lane < side if m % 2 == 0 else lane >= side
            q1, q2, q3 = split3(jnp.where(own, left, pltpu.roll(left, side, 1)))
            if terms == 2:
                return jnp.concatenate([q1, q2 * first + q3 * second], axis=1)
            high = jnp.concatenate([q1, q1 * first + q2 * second], axis=1)
            rest = jnp.concatenate([q3 * first + q2 * second, jnp.zeros_like(q1)], axis=1)
            return jnp.concatenate([high, rest], axis=0)

        def applied(weights, m, at, terms):
            rows_of = x_ref[m, : terms * side, pl.ds(at, wide)]
            got = dot(weights, jnp.concatenate([rows_of] + [rows_of[:side]] * (4 - terms), axis=0))
            return got if terms == 2 else got[:side] + got[side:]

        kept_copy = pltpu.make_async_copy(kept_ref, kept_out_ref, written)
        kept_copy.start()
        for m in range(mats):
            for r in range(0, rows, 4):
                for c in range(cols):
                    piece = [in_ref[((r + k) * cols + c) * mats + m] for k in range(4)]
                    keep(m, r * here, c * wide, jnp.concatenate(piece, axis=0), 3)
        lefts = steps([pair_gram(m, 3) for m in range(0, mats, 2)], RESTART, True)
        for m in range(mats):
            weights = weights_of(lefts, m, 3)
            for c in range(cols):
                keep(m, 0, c * wide, applied(weights, m, c * wide, 3), 2)
        lefts = steps([pair_gram(m, 2) for m in range(0, mats, 2)], ITERS - RESTART, False)
        for m in range(mats):
            weights = weights_of(lefts, m, 2)
            for c in range(cols):
                y = applied(weights, m, c * wide, 2)
                for r in range(rows):
                    out_ref[(r * cols + c) * mats + m] = y[r * here : (r + 1) * here]
        kept_copy.wait()

    def call(pieces, kept):
        n, here, wide = pieces.shape
        return pl.pallas_call(
            body,
            out_shape=(
                jax.ShapeDtypeStruct(pieces.shape, pieces.dtype),
                jax.ShapeDtypeStruct(kept.shape, kept.dtype),
            ),
            in_specs=[pl.BlockSpec(memory_space=pltpu.VMEM)] * 2,
            out_specs=(pl.BlockSpec(memory_space=pltpu.VMEM), pl.BlockSpec(memory_space=pltpu.HBM)),
            scratch_shapes=[
                pltpu.VMEM((mats, 3 * here * rows, wide * cols), BF16),
                pltpu.SemaphoreType.DMA,
            ],
            compiler_params=pltpu.CompilerParams(vmem_limit_bytes=32 * 1024 * 1024),
            name="orthogonal",
        )(pieces, kept)

    return call


PARTS = 8


def fresh_momentum(grad_stack, moment_stack):
    many = grad_stack.shape[0] // PARTS

    def body(grad_ref, moment_ref, out_ref, grads, moments, arrived):
        def copies(i):
            part = pl.ds(i * many, many)
            return (
                pltpu.make_async_copy(grad_ref.at[part], grads.at[part], arrived.at[2 * i]),
                pltpu.make_async_copy(moment_ref.at[part], moments.at[part], arrived.at[2 * i + 1]),
            )

        for i in range(PARTS):
            for copy in copies(i):
                copy.start()
        for i in range(PARTS):
            for copy in copies(i):
                copy.wait()
            part = pl.ds(i * many, many)
            out_ref[part] = hold_rate * moments[part] + grads[part]

    return pl.pallas_call(
        body,
        out_shape=pltpu.VMEM(grad_stack.shape, F32),
        in_specs=[pl.BlockSpec(memory_space=pltpu.HBM)] * 2,
        out_specs=pl.BlockSpec(memory_space=pltpu.VMEM),
        scratch_shapes=[
            pltpu.VMEM(grad_stack.shape, F32),
            pltpu.VMEM(grad_stack.shape, F32),
            pltpu.SemaphoreType.DMA((2 * PARTS,)),
        ],
        compiler_params=pltpu.CompilerParams(vmem_limit_bytes=61 * 1024 * 1024),
        name="fresh_momentum",
    )(grad_stack, moment_stack)


def stepped(weight_stack, back):
    many = back.shape[0] // PARTS

    def body(weight_ref, back_ref, out_ref, made, sent):
        def copy(i):
            part = pl.ds(i * many, many)
            return pltpu.make_async_copy(made.at[part], out_ref.at[part], sent.at[i])

        for i in range(PARTS):
            part = pl.ds(i * many, many)
            made[part] = weight_ref[part] - learn_rate * back_ref[part]
            copy(i).start()
        for i in range(PARTS):
            copy(i).wait()

    return pl.pallas_call(
        body,
        out_shape=jax.ShapeDtypeStruct(back.shape, F32),
        in_specs=[pl.BlockSpec(memory_space=pltpu.VMEM)] * 2,
        out_specs=pl.BlockSpec(memory_space=pltpu.HBM),
        scratch_shapes=[pltpu.VMEM(back.shape, F32), pltpu.SemaphoreType.DMA((PARTS,))],
        compiler_params=pltpu.CompilerParams(vmem_limit_bytes=16 * 1024 * 1024),
        name="stepped",
    )(weight_stack, back)


def on_device(grad_stack, moment_stack, weight_stack):
    axes = ("rows", "cols")
    rows, cols = lax.axis_size("rows"), lax.axis_size("cols")
    new_momentum = fresh_momentum(grad_stack, moment_stack)
    pieces = lax.all_to_all(new_momentum, axes, split_axis=0, concat_axis=0, tiled=True)
    pieces, written = orthogonal(rows, cols, pieces.shape[0] // (rows * cols))(pieces, new_momentum)
    back = lax.all_to_all(pieces, axes, split_axis=0, concat_axis=0, tiled=True)
    return (stepped(weight_stack, back), written)


def solution(mesh):
    placed = (P(None, "rows", "cols"), P(None, "rows", "cols"), P(None, "rows", "cols"))
    return jax.shard_map(
        on_device,
        mesh=mesh,
        in_specs=placed,
        out_specs=(P(None, "rows", "cols"), P(None, "rows", "cols")),
        check_vma=False,
    )
```

```python
import jax
import jax.numpy as jnp
from jax import lax
from jax.experimental import pallas as pl
from jax.experimental.pallas import tpu as pltpu
from jax.sharding import PartitionSpec as P

ITERS = 5
RESTART = 3


hold_rate = 0.95
learn_rate = 1.0

F32, BF16 = jnp.float32, jnp.bfloat16


def split3(value):
    high = value.astype(BF16)
    rest = value - high.astype(F32)
    mid = rest.astype(BF16)
    return high, mid, (rest - mid.astype(F32)).astype(BF16)


def dot(a, b):
    return lax.dot_general(a, b, (((1,), (0,)), ((), ())), preferred_element_type=F32)


def dot_t(a, b):
    return lax.dot_general(a, b, (((1,), (1,)), ((), ())), preferred_element_type=F32)


def orthogonal(rows, cols, mats):
    def body(in_ref, kept_ref, out_ref, kept_out_ref, x_ref, written):
        here, wide = in_ref.shape[1], in_ref.shape[2]
        side = here * rows
        lane = lax.broadcasted_iota(jnp.int32, (side, 2 * side), 1)
        row = lax.broadcasted_iota(jnp.int32, (side, 2 * side), 0)
        eye = jnp.where((lane == row) | (lane == row + side), 1.0, 0.0).astype(F32)
        first = jnp.where(lane < side, 1.0, 0.0).astype(BF16)
        second = jnp.where(lane < side, 0.0, 1.0).astype(BF16)

        def keep(m, top, at, value, terms):
            for k, term in enumerate(split3(value)[:terms]):
                x_ref[m, pl.ds(k * side + top, value.shape[0]), pl.ds(at, value.shape[1])] = term

        def pair_gram(m, terms):
            def by_term(k, order):
                held_terms = jnp.concatenate([x_ref[k, pl.ds(t * side, side)] for t in order], axis=0)
                c = dot_t(x_ref[k, : terms * side], held_terms)
                if terms == 2:
                    return c[:side] + c[side:]
                c = c[:side] + (c[side : 2 * side] + c[2 * side :])
                tail = jnp.concatenate([c[:, 2 * side :], jnp.zeros((side, side), F32)], axis=1)
                return c[:, : 2 * side] + tail

            one, two = by_term(m, (0, 1, 2)[:terms]), by_term(m + 1, (1, 0, 2)[:terms])
            return jnp.where(lane < side, one, two) + pltpu.roll(jnp.where(lane < side, two, one), side, 1)

        def streamed(value, terms):
            v = split3(value)
            return jnp.concatenate(v[:2] if terms == 2 else [v[0], v[1], v[2], v[0]], axis=1)

        def held(value, terms):
            v = [jnp.concatenate([v * first, v * second], axis=0) for v in split3(value)[:terms]]
            high = jnp.concatenate(v[:2], axis=1)
            high = jnp.concatenate([high, high], axis=0)
            return (high,) if terms == 2 else (high, jnp.concatenate([v[0], v[2]], axis=0))

        def product(flow, weights):
            high = dot(flow[:, : 4 * side], weights[0])
            low = high[:, 2 * side :]
            if len(weights) == 2:
                low = low + dot(flow[:, 4 * side :], weights[1])
            return high[:, : 2 * side] + low

        def steps(grams, count, normed, terms):
            pairs = range(len(grams))
            for step in range(count):
                gram_held = [held(g, terms) for g in grams]
                squares = [product(streamed(grams[p], terms), gram_held[p]) for p in pairs]
                if step == 0 and normed:
                    sizes = [norms(g) for g in grams]
                    shrink = [1.0 / s for s in sizes]
                    polys = [
                        3.4445 * eye - (4.775 * shrink[p]) * grams[p] + (2.0315 * shrink[p]) * (shrink[p] * squares[p])
                        for p in pairs
                    ]
                else:
                    polys = [3.4445 * eye - 4.775 * grams[p] + 2.0315 * squares[p] for p in pairs]
                flow = [streamed(poly, terms) for poly in polys]
                last = step + 1 == count
                if step == 0:
                    mixed = None if last else [product(flow[p], gram_held[p]) for p in pairs]
                    lefts = polys
                    if normed:
                        lefts = [poly * lax.rsqrt(s) for poly, s in zip(polys, sizes)]
                        mixed = None if last else [shrink[p] * mixed[p] for p in pairs]
                elif last:
                    lefts = [product(flow[p], held(lefts[p], terms)) for p in pairs]
                else:
                    mixed = [product(flow[p], gram_held[p]) for p in pairs]
                    lefts = [product(flow[p], held(lefts[p], terms)) for p in pairs]
                if not last:
                    grams = [product(streamed(mixed[p], terms), held(polys[p], terms)) for p in pairs]
            return lefts

        def norms(gram):
            diagonal = jnp.sum(gram * eye, axis=0, keepdims=True)
            one = jnp.sum(jnp.where(lane[:1] < side, diagonal, 0.0), axis=1, keepdims=True)
            two = jnp.sum(jnp.where(lane[:1] < side, 0.0, diagonal), axis=1, keepdims=True)
            return jnp.where(lane[:1] < side, one, two) + 1e-06

        def weights_of(lefts, m, terms):
            left = lefts[m // 2]
            own = lane < side if m % 2 == 0 else lane >= side
            q1, q2, q3 = split3(jnp.where(own, left, pltpu.roll(left, side, 1)))
            if terms == 2:
                return jnp.concatenate([q1, q2 * first + q3 * second], axis=1)
            high = jnp.concatenate([q1, q1 * first + q2 * second], axis=1)
            rest = jnp.concatenate([q3 * first + q2 * second, jnp.zeros_like(q1)], axis=1)
            return jnp.concatenate([high, rest], axis=0)

        def applied(weights, m, at, terms):
            rows_of = x_ref[m, : terms * side, pl.ds(at, wide)]
            got = dot(weights, jnp.concatenate([rows_of] + [rows_of[:side]] * (4 - terms), axis=0))
            return got if terms == 2 else got[:side] + got[side:]

        kept_copy = pltpu.make_async_copy(kept_ref, kept_out_ref, written)
        kept_copy.start()
        for m in range(mats):
            for r in range(0, rows, 4):
                for c in range(cols):
                    piece = [in_ref[((r + k) * cols + c) * mats + m] for k in range(4)]
                    keep(m, r * here, c * wide, jnp.concatenate(piece, axis=0), 3)
        lefts = steps([pair_gram(m, 3) for m in range(0, mats, 2)], RESTART, True, 3)
        for m in range(mats):
            weights = weights_of(lefts, m, 3)
            for c in range(cols):
                keep(m, 0, c * wide, applied(weights, m, c * wide, 3), 2)
        lefts = steps([pair_gram(m, 2) for m in range(0, mats, 2)], ITERS - RESTART, False, 2)
        for m in range(mats):
            weights = weights_of(lefts, m, 2)
            for c in range(cols):
                y = applied(weights, m, c * wide, 2)
                for r in range(rows):
                    out_ref[(r * cols + c) * mats + m] = y[r * here : (r + 1) * here]
        kept_copy.wait()

    def call(pieces, kept):
        n, here, wide = pieces.shape
        return pl.pallas_call(
            body,
            out_shape=(
                jax.ShapeDtypeStruct(pieces.shape, pieces.dtype),
                jax.ShapeDtypeStruct(kept.shape, kept.dtype),
            ),
            in_specs=[pl.BlockSpec(memory_space=pltpu.VMEM)] * 2,
            out_specs=(pl.BlockSpec(memory_space=pltpu.VMEM), pl.BlockSpec(memory_space=pltpu.HBM)),
            scratch_shapes=[
                pltpu.VMEM((mats, 3 * here * rows, wide * cols), BF16),
                pltpu.SemaphoreType.DMA,
            ],
            compiler_params=pltpu.CompilerParams(vmem_limit_bytes=32 * 1024 * 1024),
            name="orthogonal",
        )(pieces, kept)

    return call


PARTS = 8


def fresh_momentum(grad_stack, moment_stack):
    many = grad_stack.shape[0] // PARTS

    def body(grad_ref, moment_ref, out_ref, grads, moments, arrived):
        def copies(i):
            part = pl.ds(i * many, many)
            return (
                pltpu.make_async_copy(grad_ref.at[part], grads.at[part], arrived.at[2 * i]),
                pltpu.make_async_copy(moment_ref.at[part], moments.at[part], arrived.at[2 * i + 1]),
            )

        for i in range(PARTS):
            for copy in copies(i):
                copy.start()
        for i in range(PARTS):
            for copy in copies(i):
                copy.wait()
            part = pl.ds(i * many, many)
            out_ref[part] = hold_rate * moments[part] + grads[part]

    return pl.pallas_call(
        body,
        out_shape=pltpu.VMEM(grad_stack.shape, F32),
        in_specs=[pl.BlockSpec(memory_space=pltpu.HBM)] * 2,
        out_specs=pl.BlockSpec(memory_space=pltpu.VMEM),
        scratch_shapes=[
            pltpu.VMEM(grad_stack.shape, F32),
            pltpu.VMEM(grad_stack.shape, F32),
            pltpu.SemaphoreType.DMA((2 * PARTS,)),
        ],
        compiler_params=pltpu.CompilerParams(vmem_limit_bytes=61 * 1024 * 1024),
        name="fresh_momentum",
    )(grad_stack, moment_stack)


def stepped(weight_stack, back):
    many = back.shape[0] // PARTS

    def body(weight_ref, back_ref, out_ref, made, sent):
        def copy(i):
            part = pl.ds(i * many, many)
            return pltpu.make_async_copy(made.at[part], out_ref.at[part], sent.at[i])

        for i in range(PARTS):
            part = pl.ds(i * many, many)
            made[part] = weight_ref[part] - learn_rate * back_ref[part]
            copy(i).start()
        for i in range(PARTS):
            copy(i).wait()

    return pl.pallas_call(
        body,
        out_shape=jax.ShapeDtypeStruct(back.shape, F32),
        in_specs=[pl.BlockSpec(memory_space=pltpu.VMEM)] * 2,
        out_specs=pl.BlockSpec(memory_space=pltpu.HBM),
        scratch_shapes=[pltpu.VMEM(back.shape, F32), pltpu.SemaphoreType.DMA((PARTS,))],
        compiler_params=pltpu.CompilerParams(vmem_limit_bytes=16 * 1024 * 1024),
        name="stepped",
    )(weight_stack, back)


def on_device(grad_stack, moment_stack, weight_stack):
    axes = ("rows", "cols")
    rows, cols = lax.axis_size("rows"), lax.axis_size("cols")
    new_momentum = fresh_momentum(grad_stack, moment_stack)
    pieces = lax.all_to_all(new_momentum, axes, split_axis=0, concat_axis=0, tiled=True)
    pieces, written = orthogonal(rows, cols, pieces.shape[0] // (rows * cols))(pieces, new_momentum)
    back = lax.all_to_all(pieces, axes, split_axis=0, concat_axis=0, tiled=True)
    return (stepped(weight_stack, back), written)


def solution(mesh):
    placed = (P(None, "rows", "cols"), P(None, "rows", "cols"), P(None, "rows", "cols"))
    return jax.shard_map(
        on_device,
        mesh=mesh,
        in_specs=placed,
        out_specs=(P(None, "rows", "cols"), P(None, "rows", "cols")),
        check_vma=False,
    )
```

```python
import jax
import jax.numpy as jnp
from jax import lax
from jax.experimental import pallas as pl
from jax.experimental.pallas import tpu as pltpu
from jax.sharding import PartitionSpec as P

ITERS = 5
RESTART = 3


hold_rate = 0.95
learn_rate = 1.0

F32, BF16 = jnp.float32, jnp.bfloat16


def split3(value):
    high = value.astype(BF16)
    rest = value - high.astype(F32)
    mid = rest.astype(BF16)
    return high, mid, (rest - mid.astype(F32)).astype(BF16)


def dot(a, b):
    return lax.dot_general(a, b, (((1,), (0,)), ((), ())), preferred_element_type=F32)


def dot_t(a, b):
    return lax.dot_general(a, b, (((1,), (1,)), ((), ())), preferred_element_type=F32)


def orthogonal(rows, cols, mats):
    def body(in_ref, kept_ref, out_ref, kept_out_ref, x_ref, written):
        here, wide = in_ref.shape[1], in_ref.shape[2]
        side = here * rows
        lane = lax.broadcasted_iota(jnp.int32, (side, 2 * side), 1)
        row = lax.broadcasted_iota(jnp.int32, (side, 2 * side), 0)
        eye = jnp.where((lane == row) | (lane == row + side), 1.0, 0.0).astype(F32)
        first = jnp.where(lane < side, 1.0, 0.0).astype(BF16)
        second = jnp.where(lane < side, 0.0, 1.0).astype(BF16)

        def keep(m, top, at, value, terms):
            for k, term in enumerate(split3(value)[:terms]):
                x_ref[m, pl.ds(k * side + top, value.shape[0]), pl.ds(at, value.shape[1])] = term

        def pair_gram(m, terms):
            def by_term(k, order):
                held_terms = jnp.concatenate([x_ref[k, pl.ds(t * side, side)] for t in order], axis=0)
                c = dot_t(x_ref[k, : terms * side], held_terms)
                if terms == 2:
                    return c[:side] + c[side:]
                c = c[:side] + (c[side : 2 * side] + c[2 * side :])
                tail = jnp.concatenate([c[:, 2 * side :], jnp.zeros((side, side), F32)], axis=1)
                return c[:, : 2 * side] + tail

            one, two = by_term(m, (0, 1, 2)[:terms]), by_term(m + 1, (1, 0, 2)[:terms])
            return jnp.where(lane < side, one, two) + pltpu.roll(jnp.where(lane < side, two, one), side, 1)

        def streamed(value, terms):
            v = split3(value)
            return jnp.concatenate(v[:2] if terms == 2 else [v[0], v[1], v[2], v[0]], axis=1)

        def held(value, terms):
            v = [jnp.concatenate([v * first, v * second], axis=0) for v in split3(value)[:terms]]
            high = jnp.concatenate(v[:2], axis=1)
            high = jnp.concatenate([high, high], axis=0)
            if terms == 3:
                tail = jnp.concatenate([v[0], v[2]], axis=0)
                high = jnp.concatenate([high, jnp.concatenate([tail, jnp.zeros_like(tail)], axis=1)], axis=0)
            return high

        def product(flow, weights):
            got = dot(flow, weights)
            return got[:, : 2 * side] + got[:, 2 * side :]

        def steps(grams, count, normed, terms):
            pairs = range(len(grams))
            for step in range(count):
                gram_held = [held(g, terms) for g in grams]
                squares = [product(streamed(grams[p], terms), gram_held[p]) for p in pairs]
                if step == 0 and normed:
                    sizes = [norms(g) for g in grams]
                    shrink = [1.0 / s for s in sizes]
                    polys = [
                        3.4445 * eye - (4.775 * shrink[p]) * grams[p] + (2.0315 * shrink[p]) * (shrink[p] * squares[p])
                        for p in pairs
                    ]
                else:
                    polys = [3.4445 * eye - 4.775 * grams[p] + 2.0315 * squares[p] for p in pairs]
                flow = [streamed(poly, terms) for poly in polys]
                last = step + 1 == count
                if step == 0:
                    mixed = None if last else [product(flow[p], gram_held[p]) for p in pairs]
                    lefts = polys
                    if normed:
                        lefts = [poly * lax.rsqrt(s) for poly, s in zip(polys, sizes)]
                        mixed = None if last else [shrink[p] * mixed[p] for p in pairs]
                elif last:
                    lefts = [product(flow[p], held(lefts[p], terms)) for p in pairs]
                else:
                    mixed = [product(flow[p], gram_held[p]) for p in pairs]
                    lefts = [product(flow[p], held(lefts[p], terms)) for p in pairs]
                if not last:
                    grams = [product(streamed(mixed[p], terms), held(polys[p], terms)) for p in pairs]
            return lefts

        def norms(gram):
            diagonal = jnp.sum(gram * eye, axis=0, keepdims=True)
            one = jnp.sum(jnp.where(lane[:1] < side, diagonal, 0.0), axis=1, keepdims=True)
            two = jnp.sum(jnp.where(lane[:1] < side, 0.0, diagonal), axis=1, keepdims=True)
            return jnp.where(lane[:1] < side, one, two) + 1e-06

        def weights_of(lefts, m, terms):
            left = lefts[m // 2]
            own = lane < side if m % 2 == 0 else lane >= side
            q1, q2, q3 = split3(jnp.where(own, left, pltpu.roll(left, side, 1)))
            if terms == 2:
                return jnp.concatenate([q1, q2 * first + q3 * second], axis=1)
            high = jnp.concatenate([q1, q1 * first + q2 * second], axis=1)
            rest = jnp.concatenate([q3 * first + q2 * second, jnp.zeros_like(q1)], axis=1)
            return jnp.concatenate([high, rest], axis=0)

        def applied(weights, m, at, terms):
            rows_of = x_ref[m, : terms * side, pl.ds(at, wide)]
            got = dot(weights, jnp.concatenate([rows_of] + [rows_of[:side]] * (4 - terms), axis=0))
            return got if terms == 2 else got[:side] + got[side:]

        kept_copy = pltpu.make_async_copy(kept_ref, kept_out_ref, written)
        kept_copy.start()
        for m in range(mats):
            for r in range(0, rows, 4):
                for c in range(cols):
                    piece = [in_ref[((r + k) * cols + c) * mats + m] for k in range(4)]
                    keep(m, r * here, c * wide, jnp.concatenate(piece, axis=0), 3)
        lefts = steps([pair_gram(m, 3) for m in range(0, mats, 2)], RESTART, True, 3)
        for m in range(mats):
            weights = weights_of(lefts, m, 3)
            for c in range(cols):
                keep(m, 0, c * wide, applied(weights, m, c * wide, 3), 2)
        lefts = steps([pair_gram(m, 2) for m in range(0, mats, 2)], ITERS - RESTART, False, 2)
        for m in range(mats):
            weights = weights_of(lefts, m, 2)
            for c in range(cols):
                y = applied(weights, m, c * wide, 2)
                for r in range(rows):
                    out_ref[(r * cols + c) * mats + m] = y[r * here : (r + 1) * here]
        kept_copy.wait()

    def call(pieces, kept):
        n, here, wide = pieces.shape
        return pl.pallas_call(
            body,
            out_shape=(
                jax.ShapeDtypeStruct(pieces.shape, pieces.dtype),
                jax.ShapeDtypeStruct(kept.shape, kept.dtype),
            ),
            in_specs=[pl.BlockSpec(memory_space=pltpu.VMEM)] * 2,
            out_specs=(pl.BlockSpec(memory_space=pltpu.VMEM), pl.BlockSpec(memory_space=pltpu.HBM)),
            scratch_shapes=[
                pltpu.VMEM((mats, 3 * here * rows, wide * cols), BF16),
                pltpu.SemaphoreType.DMA,
            ],
            compiler_params=pltpu.CompilerParams(vmem_limit_bytes=32 * 1024 * 1024),
            name="orthogonal",
        )(pieces, kept)

    return call


PARTS = 8


def fresh_momentum(grad_stack, moment_stack):
    many = grad_stack.shape[0] // PARTS

    def body(grad_ref, moment_ref, out_ref, grads, moments, arrived):
        def copies(i):
            part = pl.ds(i * many, many)
            return (
                pltpu.make_async_copy(grad_ref.at[part], grads.at[part], arrived.at[2 * i]),
                pltpu.make_async_copy(moment_ref.at[part], moments.at[part], arrived.at[2 * i + 1]),
            )

        for i in range(PARTS):
            for copy in copies(i):
                copy.start()
        for i in range(PARTS):
            for copy in copies(i):
                copy.wait()
            part = pl.ds(i * many, many)
            out_ref[part] = hold_rate * moments[part] + grads[part]

    return pl.pallas_call(
        body,
        out_shape=pltpu.VMEM(grad_stack.shape, F32),
        in_specs=[pl.BlockSpec(memory_space=pltpu.HBM)] * 2,
        out_specs=pl.BlockSpec(memory_space=pltpu.VMEM),
        scratch_shapes=[
            pltpu.VMEM(grad_stack.shape, F32),
            pltpu.VMEM(grad_stack.shape, F32),
            pltpu.SemaphoreType.DMA((2 * PARTS,)),
        ],
        compiler_params=pltpu.CompilerParams(vmem_limit_bytes=61 * 1024 * 1024),
        name="fresh_momentum",
    )(grad_stack, moment_stack)


def stepped(weight_stack, back):
    many = back.shape[0] // PARTS

    def body(weight_ref, back_ref, out_ref, made, sent):
        def copy(i):
            part = pl.ds(i * many, many)
            return pltpu.make_async_copy(made.at[part], out_ref.at[part], sent.at[i])

        for i in range(PARTS):
            part = pl.ds(i * many, many)
            made[part] = weight_ref[part] - learn_rate * back_ref[part]
            copy(i).start()
        for i in range(PARTS):
            copy(i).wait()

    return pl.pallas_call(
        body,
        out_shape=jax.ShapeDtypeStruct(back.shape, F32),
        in_specs=[pl.BlockSpec(memory_space=pltpu.VMEM)] * 2,
        out_specs=pl.BlockSpec(memory_space=pltpu.HBM),
        scratch_shapes=[pltpu.VMEM(back.shape, F32), pltpu.SemaphoreType.DMA((PARTS,))],
        compiler_params=pltpu.CompilerParams(vmem_limit_bytes=16 * 1024 * 1024),
        name="stepped",
    )(weight_stack, back)


def on_device(grad_stack, moment_stack, weight_stack):
    axes = ("rows", "cols")
    rows, cols = lax.axis_size("rows"), lax.axis_size("cols")
    new_momentum = fresh_momentum(grad_stack, moment_stack)
    pieces = lax.all_to_all(new_momentum, axes, split_axis=0, concat_axis=0, tiled=True)
    pieces, written = orthogonal(rows, cols, pieces.shape[0] // (rows * cols))(pieces, new_momentum)
    back = lax.all_to_all(pieces, axes, split_axis=0, concat_axis=0, tiled=True)
    return (stepped(weight_stack, back), written)


def solution(mesh):
    placed = (P(None, "rows", "cols"), P(None, "rows", "cols"), P(None, "rows", "cols"))
    return jax.shard_map(
        on_device,
        mesh=mesh,
        in_specs=placed,
        out_specs=(P(None, "rows", "cols"), P(None, "rows", "cols")),
        check_vma=False,
    )
```

```python
import jax
import jax.numpy as jnp
from jax import lax
from jax.experimental import pallas as pl
from jax.experimental.pallas import tpu as pltpu
from jax.sharding import PartitionSpec as P

ITERS = 5
RESTART = 3


hold_rate = 0.95
learn_rate = 1.0

F32, BF16 = jnp.float32, jnp.bfloat16


def split3(value):
    high = value.astype(BF16)
    rest = value - high.astype(F32)
    mid = rest.astype(BF16)
    return high, mid, (rest - mid.astype(F32)).astype(BF16)


def dot(a, b):
    return lax.dot_general(a, b, (((1,), (0,)), ((), ())), preferred_element_type=F32)


def dot_t(a, b):
    return lax.dot_general(a, b, (((1,), (1,)), ((), ())), preferred_element_type=F32)


def orthogonal(rows, cols, mats):
    def body(in_ref, kept_ref, out_ref, kept_out_ref, *scratch):
        x_refs, written = scratch[:-1], scratch[-1]
        here, wide = in_ref.shape[1], in_ref.shape[2]
        side = here * rows
        lane = lax.broadcasted_iota(jnp.int32, (side, 2 * side), 1)
        row = lax.broadcasted_iota(jnp.int32, (side, 2 * side), 0)
        eye = jnp.where((lane == row) | (lane == row + side), 1.0, 0.0).astype(F32)
        first = jnp.where(lane < side, 1.0, 0.0).astype(BF16)
        second = jnp.where(lane < side, 0.0, 1.0).astype(BF16)

        def keep(m, top, at, value, terms):
            for k, term in enumerate(split3(value)[:terms]):
                x_refs[m][pl.ds(k * side + top, value.shape[0]), pl.ds(at, value.shape[1])] = term

        def pair_gram(m, terms):
            def by_term(k, order):
                held_terms = jnp.concatenate([x_refs[k][pl.ds(t * side, side)] for t in order], axis=0)
                c = dot_t(x_refs[k][: terms * side], held_terms)
                if terms == 2:
                    return c[:side] + c[side:]
                c = c[:side] + (c[side : 2 * side] + c[2 * side :])
                tail = jnp.concatenate([c[:, 2 * side :], jnp.zeros((side, side), F32)], axis=1)
                return c[:, : 2 * side] + tail

            one, two = by_term(m, (0, 1, 2)[:terms]), by_term(m + 1, (1, 0, 2)[:terms])
            return jnp.where(lane < side, one, two) + pltpu.roll(jnp.where(lane < side, two, one), side, 1)

        def streamed(value, terms):
            v = split3(value)
            return jnp.concatenate(v[:2] if terms == 2 else [v[0], v[1], v[2], v[0]], axis=1)

        def held(value, terms):
            v = [jnp.concatenate([v * first, v * second], axis=0) for v in split3(value)[:terms]]
            high = jnp.concatenate(v[:2], axis=1)
            high = jnp.concatenate([high, high], axis=0)
            return (high,) if terms == 2 else (high, jnp.concatenate([v[0], v[2]], axis=0))

        def product(flow, weights):
            high = dot(flow[:, : 4 * side], weights[0])
            low = high[:, 2 * side :]
            if len(weights) == 2:
                low = low + dot(flow[:, 4 * side :], weights[1])
            return high[:, : 2 * side] + low

        def steps(gram, count, normed, terms, box):
            for step in range(count):
                gram_held = held(gram, terms)
                square = product(streamed(gram, terms), gram_held)
                if step == 0 and normed:
                    size = norms(gram)
                    shrink = 1.0 / size
                yield
                if step == 0 and normed:
                    poly = 3.4445 * eye - (4.775 * shrink) * gram + (2.0315 * shrink) * (shrink * square)
                else:
                    poly = 3.4445 * eye - 4.775 * gram + 2.0315 * square
                flow = streamed(poly, terms)
                last = step + 1 == count
                if not last:
                    mixed = product(flow, gram_held)
                    if step == 0 and normed:
                        mixed = shrink * mixed
                if step == 0:
                    left = poly * lax.rsqrt(size) if normed else poly
                else:
                    left = product(flow, held(left, terms))
                yield
                if not last:
                    gram = product(streamed(mixed, terms), held(poly, terms))
                    yield
            box.append(left)

        def norms(gram):
            diagonal = jnp.sum(gram * eye, axis=0, keepdims=True)
            one = jnp.sum(jnp.where(lane[:1] < side, diagonal, 0.0), axis=1, keepdims=True)
            two = jnp.sum(jnp.where(lane[:1] < side, 0.0, diagonal), axis=1, keepdims=True)
            return jnp.where(lane[:1] < side, one, two) + 1e-06

        def weights_of(left, m, terms):
            own = lane < side if m % 2 == 0 else lane >= side
            q1, q2, q3 = split3(jnp.where(own, left, pltpu.roll(left, side, 1)))
            if terms == 2:
                return jnp.concatenate([q1, q2 * first + q3 * second], axis=1)
            high = jnp.concatenate([q1, q1 * first + q2 * second], axis=1)
            rest = jnp.concatenate([q3 * first + q2 * second, jnp.zeros_like(q1)], axis=1)
            return jnp.concatenate([high, rest], axis=0)

        def applied(weights, m, at, terms):
            rows_of = x_refs[m][: terms * side, pl.ds(at, wide)]
            got = dot(weights, jnp.concatenate([rows_of] + [rows_of[:side]] * (4 - terms), axis=0))
            return got if terms == 2 else got[:side] + got[side:]

        kept_copy = pltpu.make_async_copy(kept_ref, kept_out_ref, written)
        kept_copy.start()
        def pair(p):
            both, box = (2 * p, 2 * p + 1), []
            for c in range(cols):
                for m in both:
                    for r in range(0, rows, 4):
                        piece = [in_ref[((r + k) * cols + c) * mats + m] for k in range(4)]
                        keep(m, r * here, c * wide, jnp.concatenate(piece, axis=0), 3)
            yield
            gram = pair_gram(2 * p, 3)
            yield
            yield from steps(gram, RESTART, True, 3, box)
            weights = [weights_of(box[0], m, 3) for m in both]
            for c in range(cols):
                for w, m in zip(weights, both):
                    keep(m, 0, c * wide, applied(w, m, c * wide, 3), 2)
            yield
            gram = pair_gram(2 * p, 2)
            yield
            yield from steps(gram, ITERS - RESTART, False, 2, box)
            weights = [weights_of(box[1], m, 2) for m in both]
            for c in range(cols):
                for w, m in zip(weights, both):
                    y = applied(w, m, c * wide, 2)
                    for r in range(rows):
                        out_ref[(r * cols + c) * mats + m] = y[r * here : (r + 1) * here]
            yield

        for _ in zip(*[pair(p) for p in range(mats // 2)]):
            pass
        kept_copy.wait()

    def call(pieces, kept):
        n, here, wide = pieces.shape
        return pl.pallas_call(
            body,
            out_shape=(
                jax.ShapeDtypeStruct(pieces.shape, pieces.dtype),
                jax.ShapeDtypeStruct(kept.shape, kept.dtype),
            ),
            in_specs=[pl.BlockSpec(memory_space=pltpu.VMEM)] * 2,
            out_specs=(pl.BlockSpec(memory_space=pltpu.VMEM), pl.BlockSpec(memory_space=pltpu.HBM)),
            scratch_shapes=[
                *[pltpu.VMEM((3 * here * rows, wide * cols), BF16)] * mats,
                pltpu.SemaphoreType.DMA,
            ],
            compiler_params=pltpu.CompilerParams(vmem_limit_bytes=32 * 1024 * 1024),
            name="orthogonal",
        )(pieces, kept)

    return call


PARTS = 8


def fresh_momentum(grad_stack, moment_stack):
    many = grad_stack.shape[0] // PARTS

    def body(grad_ref, moment_ref, out_ref, grads, moments, arrived):
        def copies(i):
            part = pl.ds(i * many, many)
            return (
                pltpu.make_async_copy(grad_ref.at[part], grads.at[part], arrived.at[2 * i]),
                pltpu.make_async_copy(moment_ref.at[part], moments.at[part], arrived.at[2 * i + 1]),
            )

        for i in range(PARTS):
            for copy in copies(i):
                copy.start()
        for i in range(PARTS):
            for copy in copies(i):
                copy.wait()
            part = pl.ds(i * many, many)
            out_ref[part] = hold_rate * moments[part] + grads[part]

    return pl.pallas_call(
        body,
        out_shape=pltpu.VMEM(grad_stack.shape, F32),
        in_specs=[pl.BlockSpec(memory_space=pltpu.HBM)] * 2,
        out_specs=pl.BlockSpec(memory_space=pltpu.VMEM),
        scratch_shapes=[
            pltpu.VMEM(grad_stack.shape, F32),
            pltpu.VMEM(grad_stack.shape, F32),
            pltpu.SemaphoreType.DMA((2 * PARTS,)),
        ],
        compiler_params=pltpu.CompilerParams(vmem_limit_bytes=61 * 1024 * 1024),
        name="fresh_momentum",
    )(grad_stack, moment_stack)


def stepped(weight_stack, back):
    many = back.shape[0] // PARTS

    def body(weight_ref, back_ref, out_ref, made, sent):
        def copy(i):
            part = pl.ds(i * many, many)
            return pltpu.make_async_copy(made.at[part], out_ref.at[part], sent.at[i])

        for i in range(PARTS):
            part = pl.ds(i * many, many)
            made[part] = weight_ref[part] - learn_rate * back_ref[part]
            copy(i).start()
        for i in range(PARTS):
            copy(i).wait()

    return pl.pallas_call(
        body,
        out_shape=jax.ShapeDtypeStruct(back.shape, F32),
        in_specs=[pl.BlockSpec(memory_space=pltpu.VMEM)] * 2,
        out_specs=pl.BlockSpec(memory_space=pltpu.HBM),
        scratch_shapes=[pltpu.VMEM(back.shape, F32), pltpu.SemaphoreType.DMA((PARTS,))],
        compiler_params=pltpu.CompilerParams(vmem_limit_bytes=16 * 1024 * 1024),
        name="stepped",
    )(weight_stack, back)


def on_device(grad_stack, moment_stack, weight_stack):
    axes = ("rows", "cols")
    rows, cols = lax.axis_size("rows"), lax.axis_size("cols")
    new_momentum = fresh_momentum(grad_stack, moment_stack)
    pieces = lax.all_to_all(new_momentum, axes, split_axis=0, concat_axis=0, tiled=True)
    pieces, written = orthogonal(rows, cols, pieces.shape[0] // (rows * cols))(pieces, new_momentum)
    back = lax.all_to_all(pieces, axes, split_axis=0, concat_axis=0, tiled=True)
    return (stepped(weight_stack, back), written)


def solution(mesh):
    placed = (P(None, "rows", "cols"), P(None, "rows", "cols"), P(None, "rows", "cols"))
    return jax.shard_map(
        on_device,
        mesh=mesh,
        in_specs=placed,
        out_specs=(P(None, "rows", "cols"), P(None, "rows", "cols")),
        check_vma=False,
    )
```

```python
import jax
import jax.numpy as jnp
from jax import lax
from jax.experimental import pallas as pl
from jax.experimental.pallas import tpu as pltpu
from jax.sharding import PartitionSpec as P

ITERS = 5
RESTART = 3


hold_rate = 0.95
learn_rate = 1.0

F32, BF16 = jnp.float32, jnp.bfloat16


def split3(value):
    high = value.astype(BF16)
    rest = value - high.astype(F32)
    mid = rest.astype(BF16)
    return high, mid, (rest - mid.astype(F32)).astype(BF16)


def dot(a, b):
    return lax.dot_general(a, b, (((1,), (0,)), ((), ())), preferred_element_type=F32)


def dot_t(a, b):
    return lax.dot_general(a, b, (((1,), (1,)), ((), ())), preferred_element_type=F32)


def orthogonal(rows, cols, mats):
    def body(in_ref, kept_ref, far_ref, out_ref, kept_out_ref, near_ref, x_ref, written, fetched):
        here, wide = in_ref.shape[1], in_ref.shape[2]
        side = here * rows
        lane = lax.broadcasted_iota(jnp.int32, (side, 2 * side), 1)
        row = lax.broadcasted_iota(jnp.int32, (side, 2 * side), 0)
        eye = jnp.where((lane == row) | (lane == row + side), 1.0, 0.0).astype(F32)
        first = jnp.where(lane < side, 1.0, 0.0).astype(BF16)
        second = jnp.where(lane < side, 0.0, 1.0).astype(BF16)

        def keep(m, top, at, value, terms):
            for k, term in enumerate(split3(value)[:terms]):
                x_ref[m, pl.ds(k * side + top, value.shape[0]), pl.ds(at, value.shape[1])] = term

        def pair_gram(m, terms):
            def by_term(k, order):
                held_terms = jnp.concatenate([x_ref[k, pl.ds(t * side, side)] for t in order], axis=0)
                c = dot_t(x_ref[k, : terms * side], held_terms)
                if terms == 2:
                    return c[:side] + c[side:]
                c = c[:side] + (c[side : 2 * side] + c[2 * side :])
                tail = jnp.concatenate([c[:, 2 * side :], jnp.zeros((side, side), F32)], axis=1)
                return c[:, : 2 * side] + tail

            one, two = by_term(m, (0, 1, 2)[:terms]), by_term(m + 1, (1, 0, 2)[:terms])
            return jnp.where(lane < side, one, two) + pltpu.roll(jnp.where(lane < side, two, one), side, 1)

        def streamed(value, terms):
            v = split3(value)
            return jnp.concatenate(v[:2] if terms == 2 else [v[0], v[1], v[2], v[0]], axis=1)

        def held(value, terms):
            v = [jnp.concatenate([v * first, v * second], axis=0) for v in split3(value)[:terms]]
            high = jnp.concatenate(v[:2], axis=1)
            high = jnp.concatenate([high, high], axis=0)
            return (high,) if terms == 2 else (high, jnp.concatenate([v[0], v[2]], axis=0))

        def product(flow, weights):
            high = dot(flow[:, : 4 * side], weights[0])
            low = high[:, 2 * side :]
            if len(weights) == 2:
                low = low + dot(flow[:, 4 * side :], weights[1])
            return high[:, : 2 * side] + low

        def steps(grams, count, normed, terms):
            pairs = range(len(grams))
            for step in range(count):
                gram_held = [held(g, terms) for g in grams]
                squares = [product(streamed(grams[p], terms), gram_held[p]) for p in pairs]
                if step == 0 and normed:
                    sizes = [norms(g) for g in grams]
                    shrink = [1.0 / s for s in sizes]
                    polys = [
                        3.4445 * eye - (4.775 * shrink[p]) * grams[p] + (2.0315 * shrink[p]) * (shrink[p] * squares[p])
                        for p in pairs
                    ]
                else:
                    polys = [3.4445 * eye - 4.775 * grams[p] + 2.0315 * squares[p] for p in pairs]
                flow = [streamed(poly, terms) for poly in polys]
                last = step + 1 == count
                if step == 0:
                    mixed = None if last else [product(flow[p], gram_held[p]) for p in pairs]
                    lefts = polys
                    if normed:
                        lefts = [poly * lax.rsqrt(s) for poly, s in zip(polys, sizes)]
                        mixed = None if last else [shrink[p] * mixed[p] for p in pairs]
                elif last:
                    lefts = [product(flow[p], held(lefts[p], terms)) for p in pairs]
                else:
                    mixed = [product(flow[p], gram_held[p]) for p in pairs]
                    lefts = [product(flow[p], held(lefts[p], terms)) for p in pairs]
                if not last:
                    grams = [product(streamed(mixed[p], terms), held(polys[p], terms)) for p in pairs]
            return lefts

        def norms(gram):
            diagonal = jnp.sum(gram * eye, axis=0, keepdims=True)
            one = jnp.sum(jnp.where(lane[:1] < side, diagonal, 0.0), axis=1, keepdims=True)
            two = jnp.sum(jnp.where(lane[:1] < side, 0.0, diagonal), axis=1, keepdims=True)
            return jnp.where(lane[:1] < side, one, two) + 1e-06

        def weights_of(lefts, m, terms):
            left = lefts[m // 2]
            own = lane < side if m % 2 == 0 else lane >= side
            q1, q2, q3 = split3(jnp.where(own, left, pltpu.roll(left, side, 1)))
            if terms == 2:
                return jnp.concatenate([q1, q2 * first + q3 * second], axis=1)
            high = jnp.concatenate([q1, q1 * first + q2 * second], axis=1)
            rest = jnp.concatenate([q3 * first + q2 * second, jnp.zeros_like(q1)], axis=1)
            return jnp.concatenate([high, rest], axis=0)

        def applied(weights, m, at, terms):
            rows_of = x_ref[m, : terms * side, pl.ds(at, wide)]
            got = dot(weights, jnp.concatenate([rows_of] + [rows_of[:side]] * (4 - terms), axis=0))
            return got if terms == 2 else got[:side] + got[side:]

        kept_copy = pltpu.make_async_copy(kept_ref, kept_out_ref, written)
        kept_copy.start()
        fetch = pltpu.make_async_copy(far_ref, near_ref, fetched)
        fetch.start()
        for m in range(mats):
            for r in range(0, rows, 4):
                for c in range(cols):
                    piece = [in_ref[((r + k) * cols + c) * mats + m] for k in range(4)]
                    keep(m, r * here, c * wide, jnp.concatenate(piece, axis=0), 3)
        lefts = steps([pair_gram(m, 3) for m in range(0, mats, 2)], RESTART, True, 3)
        for m in range(mats):
            weights = weights_of(lefts, m, 3)
            for c in range(cols):
                keep(m, 0, c * wide, applied(weights, m, c * wide, 3), 2)
        lefts = steps([pair_gram(m, 2) for m in range(0, mats, 2)], ITERS - RESTART, False, 2)
        for m in range(mats):
            weights = weights_of(lefts, m, 2)
            for c in range(cols):
                y = applied(weights, m, c * wide, 2)
                for r in range(rows):
                    out_ref[(r * cols + c) * mats + m] = y[r * here : (r + 1) * here]
        kept_copy.wait()
        fetch.wait()

    def call(pieces, kept, far):
        n, here, wide = pieces.shape
        return pl.pallas_call(
            body,
            out_shape=(
                jax.ShapeDtypeStruct(pieces.shape, pieces.dtype),
                jax.ShapeDtypeStruct(kept.shape, kept.dtype),
                pltpu.VMEM(far.shape, far.dtype),
            ),
            in_specs=[pl.BlockSpec(memory_space=pltpu.VMEM)] * 2 + [pl.BlockSpec(memory_space=pltpu.HBM)],
            out_specs=(
                pl.BlockSpec(memory_space=pltpu.VMEM),
                pl.BlockSpec(memory_space=pltpu.HBM),
                pl.BlockSpec(memory_space=pltpu.VMEM),
            ),
            scratch_shapes=[
                pltpu.VMEM((mats, 3 * here * rows, wide * cols), BF16),
                pltpu.SemaphoreType.DMA,
                pltpu.SemaphoreType.DMA,
            ],
            compiler_params=pltpu.CompilerParams(vmem_limit_bytes=32 * 1024 * 1024),
            name="orthogonal",
        )(pieces, kept, far)

    return call


PARTS = 8


def fresh_momentum(grad_stack, moment_stack):
    many = grad_stack.shape[0] // PARTS

    def body(grad_ref, moment_ref, out_ref, grads, moments, arrived):
        def copies(i):
            part = pl.ds(i * many, many)
            return (
                pltpu.make_async_copy(grad_ref.at[part], grads.at[part], arrived.at[2 * i]),
                pltpu.make_async_copy(moment_ref.at[part], moments.at[part], arrived.at[2 * i + 1]),
            )

        for i in range(PARTS):
            for copy in copies(i):
                copy.start()
        for i in range(PARTS):
            for copy in copies(i):
                copy.wait()
            part = pl.ds(i * many, many)
            out_ref[part] = hold_rate * moments[part] + grads[part]

    return pl.pallas_call(
        body,
        out_shape=pltpu.VMEM(grad_stack.shape, F32),
        in_specs=[pl.BlockSpec(memory_space=pltpu.HBM)] * 2,
        out_specs=pl.BlockSpec(memory_space=pltpu.VMEM),
        scratch_shapes=[
            pltpu.VMEM(grad_stack.shape, F32),
            pltpu.VMEM(grad_stack.shape, F32),
            pltpu.SemaphoreType.DMA((2 * PARTS,)),
        ],
        compiler_params=pltpu.CompilerParams(vmem_limit_bytes=61 * 1024 * 1024),
        name="fresh_momentum",
    )(grad_stack, moment_stack)


def stepped(weight_stack, back):
    many = back.shape[0] // PARTS

    def body(weight_ref, back_ref, out_ref, made, sent):
        def copy(i):
            part = pl.ds(i * many, many)
            return pltpu.make_async_copy(made.at[part], out_ref.at[part], sent.at[i])

        for i in range(PARTS):
            part = pl.ds(i * many, many)
            made[part] = weight_ref[part] - learn_rate * back_ref[part]
            copy(i).start()
        for i in range(PARTS):
            copy(i).wait()

    return pl.pallas_call(
        body,
        out_shape=jax.ShapeDtypeStruct(back.shape, F32),
        in_specs=[pl.BlockSpec(memory_space=pltpu.VMEM)] * 2,
        out_specs=pl.BlockSpec(memory_space=pltpu.HBM),
        scratch_shapes=[pltpu.VMEM(back.shape, F32), pltpu.SemaphoreType.DMA((PARTS,))],
        compiler_params=pltpu.CompilerParams(vmem_limit_bytes=16 * 1024 * 1024),
        name="stepped",
    )(weight_stack, back)


def on_device(grad_stack, moment_stack, weight_stack):
    axes = ("rows", "cols")
    rows, cols = lax.axis_size("rows"), lax.axis_size("cols")
    new_momentum = fresh_momentum(grad_stack, moment_stack)
    pieces = lax.all_to_all(new_momentum, axes, split_axis=0, concat_axis=0, tiled=True)
    pieces, written, weights = orthogonal(rows, cols, pieces.shape[0] // (rows * cols))(pieces, new_momentum, weight_stack)
    back = lax.all_to_all(pieces, axes, split_axis=0, concat_axis=0, tiled=True)
    return (stepped(weights, back), written)


def solution(mesh):
    placed = (P(None, "rows", "cols"), P(None, "rows", "cols"), P(None, "rows", "cols"))
    return jax.shard_map(
        on_device,
        mesh=mesh,
        in_specs=placed,
        out_specs=(P(None, "rows", "cols"), P(None, "rows", "cols")),
        check_vma=False,
    )
```
